256 devices in a mesh: rep: 4 (over y, x), bx: 64 (over z, core).
Axes of the slice: x: 2, y: 2, z: 32, core: 2. Of those that a mesh axis runs over, the one named last changes fastest.
The devices are a block of a 4x8x32 slice.
Arguments:
- positions: float32 [1024, 3, 128], P(('rep', 'bx')), parts along dimension 0, may hold values from 0 to 4.5
- species: int32 [1024, 128], P(('rep', 'bx')), parts along dimension 0, may hold values from 0 to 88
- element_embed: bfloat16 [89, 128], replicated, may hold values from -6 to 6
- radial_one: float32 [8, 128], replicated, may hold values from -2 to 2
- mix_one: bfloat16 [128, 128], replicated, may hold values from -0.5 to 0.5
- radial_two: float32 [8, 128], replicated, may hold values from -2 to 2
- mix_two: bfloat16 [128, 128], replicated, may hold values from -0.5 to 0.5
- readout: bfloat16 [128], replicated, may hold values from -0.5 to 0.5
- tile_list: int32 [3072, 2], P(('rep', 'bx')), parts along dimension 0, may hold values from 0 to 7, as said below
- tile_count: int32 [256], P(('rep', 'bx')), parts along dimension 0, may hold values from 4 to 12, as said below
- border: int32 [512, 2], P(('rep', 'bx')), parts along dimension 0, may hold values from 0 to 3, as said below
Outputs:
- atom_energy: float32 [1024, 128], P(('rep', 'bx')), parts along dimension 0
- forces: float32 [1024, 3, 128], P(('rep', 'bx')), parts along dimension 0
- descriptors: bfloat16 [1024, 4, 128, 128], P(('rep', 'bx')), parts along dimension 0
The draws below stay inside these ranges and needn't reach their ends.
There are 4 independent parts, one for each index of `rep`. The reference program is written for one: setup_inputs(seed, part) draws one part's arguments, and reference() takes and returns one part's arrays. A program takes and returns all parts, laid end to end along the dimension named above; an argument that names none is the same for every part. Nothing has to cross between parts.
Inputs may be any that keep to these rules, and one draw needn't show every extreme that they name: `tile_list`: row 12 d + t belongs to slab d: its first entry is a cluster of that slab (0 to 3), its second a position in ext_d (0 to 7). `tile_count`: live tiles of a slab; 12 on at least one slab of every draw. `border`: rows 2 d and 2 d + 1 list distinct clusters of slab d, sent to its left and to its right neighbour.
All inputs are finite; a program needn't handle non-finite values.
Results may differ from the reference program's by a relative error of at most 0.0058.
Values may be sent and summed in bfloat16 or wider, within the bound.
A program may use at most 64 MiB of HBM per device.

```python
import jax
import jax.numpy as jnp
from jax import lax

CHANNELS = 128
BASES = 8
ELEMENTS = 89
CLUSTER = 128
CL_DEV = 4
BORDER = 2
TILE_CAP = 12
CLUSTERS = 256
N_BX = 64


def draw_tile_list(key, part):
    key_center, key_partner = jax.random.split(jax.random.fold_in(key, 23))
    center = jax.random.randint(key_center, (N_BX * TILE_CAP, 1), 0, CL_DEV)
    partner = jax.random.randint(key_partner, (N_BX * TILE_CAP, 1), 0, CL_DEV + 2 * BORDER)
    return jnp.concatenate([center, partner], axis=1).astype(jnp.int32)


def draw_tile_count(key, part):
    key_heated, key_forced, key_normal = jax.random.split(jax.random.fold_in(key, 11), 3)
    forced = jax.random.randint(key_forced, (), 0, N_BX)
    heated = (jax.random.randint(key_heated, (N_BX,), 0, 8) == 0) | (jnp.arange(N_BX) == forced)
    normal_count = CL_DEV + jax.random.randint(key_normal, (N_BX,), 0, CL_DEV // 2 + 1)
    return jnp.where(heated, TILE_CAP, normal_count).astype(jnp.int32)


def draw_border(key, part):
    scores = jax.random.randint(jax.random.fold_in(key, 37), (2 * N_BX, CL_DEV), 0, 2 ** 20)
    ranking = scores * CL_DEV + jnp.arange(CL_DEV, dtype=jnp.int32)[None]
    ordering = jnp.argsort(ranking, axis=1, stable=True)
    return ordering[:, :BORDER].astype(jnp.int32)


def plant(result, own_key, smallest, top_value):
    shape = result.shape
    spot = [jax.random.randint(jax.random.fold_in(own_key, axis), (), 0, shape[axis]) for axis in range(len(shape))]
    result = result.at[tuple(spot)].set(smallest)
    longest = shape.index(max(shape))
    spot[longest] = (spot[longest] + 1) % shape[longest]
    return result.at[tuple(spot)].set(top_value)


def level_of(own_key, shape, cuts, low, largest):
    def one(axis_at, parts):
        steps = jax.random.uniform(jax.random.fold_in(jax.random.fold_in(own_key, 6), axis_at), (parts,), jnp.float32, low / len(cuts), largest / len(cuts))
        return jnp.repeat(jnp.exp(steps), shape[axis_at] // parts).reshape((-1,) + (1,) * (len(shape) - axis_at - 1))

    gain = one(*cuts[0])
    for cut in cuts[1:]:
        gain = gain * one(*cut)
    return gain


def noise(stream_key, shape, scale, bound, kind=jnp.bfloat16):
    return jnp.clip(scale * jax.random.normal(stream_key, shape, jnp.float32), -bound, bound).astype(kind)


def setup_inputs(seed: int = 0, part: int = 0) -> dict:
    splits = jax.random.split(jax.random.key(seed), 12)
    part_keys = jax.random.split(jax.random.fold_in(splits[11], part), 12)
    positions = jnp.clip(4.5 * jax.random.uniform(part_keys[0], (CLUSTERS, 3, CLUSTER), jnp.float32) ** level_of(part_keys[0], (CLUSTERS, 3, CLUSTER), ((0, 64),), -0.2, 0.2), 0.0, 4.5)
    species = plant(jax.random.randint(part_keys[1], (CLUSTERS, CLUSTER), 0, ELEMENTS), jax.random.fold_in(part_keys[1], 1), 0, ELEMENTS - 1).astype(jnp.int32)
    element_embed = noise(splits[2], (ELEMENTS, CHANNELS), 1.0, 6.0)
    radial_one = noise(splits[3], (BASES, CHANNELS), BASES ** -0.5, 2.0, jnp.float32)
    mix_one = noise(splits[4], (CHANNELS, CHANNELS), CHANNELS ** -0.5, 0.5)
    radial_two = noise(splits[5], (BASES, CHANNELS), BASES ** -0.5, 2.0, jnp.float32)
    mix_two = noise(splits[6], (CHANNELS, CHANNELS), CHANNELS ** -0.5, 0.5)
    readout = noise(splits[7], (CHANNELS,), CHANNELS ** -0.5, 0.5)
    tile_list = draw_tile_list(jax.random.fold_in(jax.random.fold_in(splits[11], part), 71), part)
    tile_count = draw_tile_count(jax.random.fold_in(jax.random.fold_in(splits[11], part), 71), part)
    border = draw_border(jax.random.fold_in(jax.random.fold_in(splits[11], part), 71), part)
    return {"positions": positions, "species": species, "element_embed": element_embed, "radial_one": radial_one, "mix_one": mix_one, "radial_two": radial_two, "mix_two": mix_two, "readout": readout, "tile_list": tile_list, "tile_count": tile_count, "border": border}


soften = 0.25
cutoff = 3.6
spread = 0.9
first_center = 0.25
center_step = 0.45
message_scale = 0.125
highest = lax.Precision.HIGHEST

def rounded(value):
    return lax.optimization_barrier(value.astype(jnp.bfloat16)).astype(jnp.float32)

def geometry(pos_center, pos_partner, same_cluster):
    offset = pos_partner[:, None, :] - pos_center[:, :, None]
    radius = jnp.sqrt(lax.optimization_barrier(jnp.sum(offset * offset, axis=0)) + soften)
    direction = offset / radius[None]
    cluster_size = radius.shape[0]
    centers = first_center + center_step * jnp.arange(BASES, dtype=jnp.float32)
    envelope = jnp.square(jnp.maximum(1.0 - jnp.square(radius / cutoff), 0.0))
    diagonal = (lax.broadcasted_iota(jnp.int32, (cluster_size, cluster_size), 0) == lax.broadcasted_iota(jnp.int32, (cluster_size, cluster_size), 1)).astype(jnp.float32)
    weight_mask = envelope * (1.0 - same_cluster * diagonal)
    radial_basis = jnp.exp(-jnp.square((radius[None] - centers[:, None, None]) / spread)) * weight_mask[None]
    harmonics = jnp.concatenate([jnp.ones_like(radius)[None], direction], axis=0)
    return radial_basis[:, :, None, :] * jnp.transpose(harmonics, (1, 0, 2))[None]

def extended_index(border):
    device = jnp.arange(N_BX, dtype=jnp.int32)
    left_device = (device - 1) % N_BX
    right_device = (device + 1) % N_BX
    from_left = left_device[:, None] * CL_DEV + border[2 * left_device + 1]
    own_index = device[:, None] * CL_DEV + jnp.arange(CL_DEV, dtype=jnp.int32)[None]
    from_right = right_device[:, None] * CL_DEV + border[2 * right_device]
    return jnp.concatenate([from_left, own_index, from_right], axis=1).astype(jnp.int32)

def tile_parts(rows_here, tile_index):
    center = rows_here[tile_index, 0]
    partner = rows_here[tile_index, 1]
    same_cluster = (partner == center + BORDER).astype(jnp.float32)
    return (center, partner, same_cluster)

def geometry_pullback(pos_here, center, partner, same_cluster, kernel_grad):

    def local_geometry(center_pos, partner_pos):
        return geometry(center_pos, partner_pos, same_cluster)
    pullback = jax.vjp(local_geometry, pos_here[center + BORDER], pos_here[partner])[1]
    return pullback(kernel_grad)

def reference(positions, species, element_embed, radial_one, mix_one, radial_two, mix_two, readout, tile_list, tile_count, border):
    index_ext = extended_index(border)
    flat_index = index_ext.reshape(-1)
    extent = CL_DEV + 2 * BORDER
    onehot = (species[..., None] == jnp.arange(ELEMENTS, dtype=jnp.int32)).astype(jnp.float32)
    own_feature = jnp.einsum('xas,sc->xac', onehot, element_embed.astype(jnp.float32), precision=highest)
    tile_rows = tile_list.reshape(N_BX, TILE_CAP, 2)
    live_mask = (jnp.arange(TILE_CAP, dtype=jnp.int32)[None] < tile_count[:, None]).astype(jnp.float32)
    tile_range = jnp.arange(TILE_CAP, dtype=jnp.int32)
    mix_one_wide = mix_one.astype(jnp.float32)
    mix_two_wide = mix_two.astype(jnp.float32)
    readout_wide = readout.astype(jnp.float32)
    pos_ext = positions[index_ext]
    feat_ext = own_feature[index_ext]

    def layer_one_device(inputs):
        pos_here, feat_here, rows_here, live_here = inputs

        def tile_step(totals, tile_index):
            center, partner, same_cluster = tile_parts(rows_here, tile_index)
            kernel = rounded(geometry(pos_here[center + BORDER], pos_here[partner], same_cluster))
            product = jnp.einsum('kamb,bc->kamc', kernel, feat_here[partner], precision=highest)
            message = message_scale * lax.optimization_barrier(jnp.sum(radial_one[:, None, None, :] * product, axis=0))
            return (totals.at[center].add(live_here[tile_index] * jnp.swapaxes(message, 0, 1)), None)
        start = jnp.zeros((CL_DEV, 4, CLUSTER, CHANNELS), jnp.float32)
        return lax.scan(tile_step, start, tile_range)[0]

    def layer_two_device(inputs):
        pos_here, feature_here, rows_here, live_here = inputs

        def tile_step(totals, tile_index):
            center, partner, same_cluster = tile_parts(rows_here, tile_index)
            kernel = rounded(geometry(pos_here[center + BORDER], pos_here[partner], same_cluster))
            product = jnp.einsum('kamb,mbc->kac', kernel, feature_here[partner], precision=highest)
            message = message_scale * lax.optimization_barrier(jnp.sum(radial_two[:, None, :] * product, axis=0))
            return (totals.at[center].add(live_here[tile_index] * message), None)
        start = jnp.zeros((CL_DEV, CLUSTER, CHANNELS), jnp.float32)
        return lax.scan(tile_step, start, tile_range)[0]

    def layer_two_back_device(inputs):
        pos_here, feature_here, rows_here, live_here, adjoint_here = inputs

        def tile_step(carry, tile_index):
            feature_grad, position_grad = carry
            center, partner, same_cluster = tile_parts(rows_here, tile_index)
            live_flag = live_here[tile_index]
            kernel = rounded(geometry(pos_here[center + BORDER], pos_here[partner], same_cluster))
            weighted = rounded(message_scale * radial_two[:, None, :] * adjoint_here[center][None])
            partner_grad = jnp.einsum('kamb,kac->mbc', kernel, weighted, precision=highest)
            kernel_grad = jnp.einsum('kac,mbc->kamb', weighted, feature_here[partner], precision=highest)
            grad_center, grad_partner = geometry_pullback(pos_here, center, partner, same_cluster, live_flag * kernel_grad)
            feature_grad = feature_grad.at[partner].add(live_flag * partner_grad)
            position_grad = position_grad.at[center + BORDER].add(grad_center).at[partner].add(grad_partner)
            return ((feature_grad, position_grad), None)
        start = (jnp.zeros((extent, 4, CLUSTER, CHANNELS), jnp.float32), jnp.zeros((extent, 3, CLUSTER), jnp.float32))
        return lax.scan(tile_step, start, tile_range)[0]

    def layer_one_back_device(inputs):
        pos_here, feat_here, rows_here, live_here, adjoint_here = inputs

        def tile_step(position_grad, tile_index):
            center, partner, same_cluster = tile_parts(rows_here, tile_index)
            live_flag = live_here[tile_index]
            weighted = rounded(message_scale * radial_one[:, None, None, :] * jnp.swapaxes(adjoint_here[center], 0, 1)[None])
            kernel_grad = jnp.einsum('kamc,bc->kamb', weighted, feat_here[partner], precision=highest)
            grad_center, grad_partner = geometry_pullback(pos_here, center, partner, same_cluster, live_flag * kernel_grad)
            return (position_grad.at[center + BORDER].add(grad_center).at[partner].add(grad_partner), None)
        start = jnp.zeros((extent, 3, CLUSTER), jnp.float32)
        return lax.scan(tile_step, start, tile_range)[0]
    first_sum = lax.map(layer_one_device, (pos_ext, feat_ext, tile_rows, live_mask))
    first_sum = first_sum.reshape(CLUSTERS, 4, CLUSTER, CHANNELS)
    mixed_one = jnp.einsum('xmac,cd->xmad', rounded(first_sum), mix_one_wide, precision=highest)
    mixed_one = mixed_one.at[:, 0].add(own_feature)
    layer_feature = rounded(mixed_one)
    feature_ext = layer_feature[index_ext]
    second_sum = lax.map(layer_two_device, (pos_ext, feature_ext, tile_rows, live_mask))
    second_sum = second_sum.reshape(CLUSTERS, CLUSTER, CHANNELS)
    activation = jnp.einsum('xac,cd->xad', rounded(second_sum), mix_two_wide, precision=highest)
    activation = activation + layer_feature[:, 0] + lax.optimization_barrier(jnp.sum(jnp.square(layer_feature[:, 1:]), axis=1))
    sigmoid_z = jax.nn.sigmoid(activation)
    atom_energy = lax.optimization_barrier(jnp.sum(activation * sigmoid_z * readout_wide, axis=-1))
    energy_adjoint = readout_wide * sigmoid_z * (1.0 + activation * (1.0 - sigmoid_z))
    second_adjoint = jnp.einsum('xae,ce->xac', energy_adjoint, mix_two_wide, precision=highest)
    direct_adjoint = jnp.concatenate([energy_adjoint[:, None], 2.0 * layer_feature[:, 1:] * energy_adjoint[:, None]], axis=1)
    adjoint_blocks = second_adjoint.reshape(N_BX, CL_DEV, CLUSTER, CHANNELS)
    feature_back, moves_two = lax.map(layer_two_back_device, (pos_ext, feature_ext, tile_rows, live_mask, adjoint_blocks))
    feature_adjoint = direct_adjoint.at[flat_index].add(feature_back.reshape(-1, 4, CLUSTER, CHANNELS))
    moves_total = jnp.zeros_like(positions).at[flat_index].add(moves_two.reshape(-1, 3, CLUSTER))
    first_adjoint = jnp.einsum('xmae,ce->xmac', feature_adjoint, mix_one_wide, precision=highest)
    first_blocks = first_adjoint.reshape(N_BX, CL_DEV, 4, CLUSTER, CHANNELS)
    moves_one = lax.map(layer_one_back_device, (pos_ext, feat_ext, tile_rows, live_mask, first_blocks))
    moves_total = moves_total.at[flat_index].add(moves_one.reshape(-1, 3, CLUSTER))
    return (atom_energy, -moves_total, layer_feature.astype(jnp.bfloat16))
```

```python
import functools
import math

import jax
import jax.numpy as jnp
from jax import lax
from jax.experimental import pallas as pl
from jax.experimental.pallas import tpu as pltpu
from jax.sharding import PartitionSpec as P

MESH = pl.DeviceIdType.MESH
F32 = jnp.float32
BF16 = jnp.bfloat16

soften = 0.25
cutoff = 3.6
spread = 0.9
first_center = 0.25
center_step = 0.45
message_scale = 0.125
ratio = center_step / spread

NN = (((1,), (0,)), ((), ()))
NT = (((1,), (1,)), ((), ()))
TN = (((0,), (0,)), ((), ()))


def dot(a, b, dims=NN):
    return lax.dot_general(a, b, dims, preferred_element_type=F32)


def split(value):
    high = value.astype(BF16)
    return high, (value - high.astype(F32)).astype(BF16)


def body(
    sizes,
    tiles_ref,
    count_ref,
    border_ref,
    pos_far,
    species_far,
    embed_far,
    radial_one_far,
    mix_one_far,
    radial_two_far,
    mix_two_far,
    readout_far,
    energy_ref,
    forces_ref,
    desc_ref,
    links,
    pos_ref,
    species_ref,
    embed_ref,
    radial_one_ref,
    mix_one_ref,
    radial_two_ref,
    mix_two_ref,
    readout_ref,
    load_sem,
    send_pos,
    recv_pos,
    send_feat,
    recv_feat,
    send_grad,
    recv_grad,
    recv_move,
    pos_ext,
    spread_pos,
    scale_one,
    scale_two,
    feat_t,
    feat,
    lift_one,
    layer_t,
    layer,
    kern,
    radial,
    direction,
    total,
    second,
    adj_two,
    adj_two_t,
    adj_one_t,
    direct,
    moves,
    send_sem,
    recv_sem,
):
    n, clusters, margin, cap, bases, size = sizes
    ext = clusters + 2 * margin
    me = lax.axis_index("bx")
    rep = lax.axis_index("rep")
    right = lax.rem(me + 1, n)
    left = lax.rem(me + n - 1, n)

    def cols(i, width=1):
        return slice(i * size, (i + width) * size)

    def exchange(step, src_left, src_right, dst):
        out = []
        for side, (src, target) in enumerate(((src_left, left), (src_right, right))):
            copy = pltpu.make_async_remote_copy(
                src_ref=src,
                dst_ref=dst[1 - side],
                send_sem=send_sem.at[step, side],
                recv_sem=recv_sem.at[step, 1 - side],
                device_id=(rep, target),
                device_id_type=MESH,
            )
            copy.start()
            out.append(copy)
        return out

    def finish(copies):
        for copy in copies:
            copy.wait()

    far = (
        pos_far, species_far, embed_far, radial_one_far, mix_one_far, radial_two_far, mix_two_far, readout_far
    )
    near = (
        pos_ref, species_ref, embed_ref, radial_one_ref, mix_one_ref, radial_two_ref, mix_two_ref, readout_ref
    )
    loads = [
        pltpu.make_async_copy(src, dst, load_sem.at[i])
        for i, (src, dst) in enumerate(zip(far, near, strict=True))
    ]
    for load in loads:
        load.start()
    barrier = pltpu.get_barrier_semaphore()
    for neighbour in (left, right):
        pl.semaphore_signal(barrier, inc=1, device_id=(rep, neighbour), device_id_type=MESH)

    for load in loads:
        load.wait()
    for side in range(2):
        for s in range(margin):
            which = border_ref[side, s]
            for e in range(3):
                send_pos[side, s, e : e + 1] = pos_ref[e, pl.ds(which, 1)]
            send_pos[side, s, 3:4] = species_ref[pl.ds(which, 1)].astype(F32)
    pl.semaphore_wait(barrier, 2)
    pos_dst = (recv_pos.at[0], recv_pos.at[1])
    pos_copies = exchange(0, send_pos.at[0], send_pos.at[1], pos_dst)

    centers = [tiles_ref[0, t] for t in range(cap)]
    partners = [tiles_ref[1, t] for t in range(cap)]
    none = jnp.int32(cap)
    for row, ids, how_many in ((0, centers, clusters), (1, partners, ext)):
        for t in range(cap):
            found = none
            for s in range(t):
                found = jnp.where(ids[s] == ids[t], jnp.int32(s), found)
            links[row, t] = found
        for g in range(how_many):
            found = none
            for s in range(cap):
                found = jnp.where(ids[s] == g, jnp.int32(s), found)
            links[2 + row, g] = found
    for side in range(2):
        for g in range(clusters):
            found = jnp.int32(margin)
            for s in range(margin):
                found = jnp.where(border_ref[side, s] == g, jnp.int32(s), found)
            links[4 + side, g] = found

    def spread_row(row):
        return jnp.broadcast_to(row, (size, size)).T

    for k in range(bases):
        scale_one[k] = message_scale * spread_row(radial_one_ref[k : k + 1])
        scale_two[k] = message_scale * spread_row(radial_two_ref[k : k + 1])
    total[cap] = jnp.zeros(total.shape[1:], F32)
    second[cap] = jnp.zeros(second.shape[1:], F32)
    for side in range(2):
        recv_grad[side, margin] = jnp.zeros(recv_grad.shape[2:], BF16)
        recv_move[side, margin] = jnp.zeros(recv_move.shape[2:], F32)
    moves[...] = jnp.zeros(moves.shape, F32)
    kinds = embed_ref.shape[0]
    kind_row = lax.broadcasted_iota(jnp.int32, (kinds, size), 0)

    def prepare(x):
        here = pos_ext[x]
        for e in range(3):
            spread_pos[x, e] = spread_row(here[e : e + 1])
        onehot = (kind_row == here[3:4].astype(jnp.int32)).astype(F32).astype(BF16)
        first = dot(embed_ref[...], onehot, TN)
        feat_t[x] = first
        feat[x] = first.T.astype(BF16)
        for k in range(bases):
            high, low = split(scale_one[k] * first)
            lift_one[x, 0:size, cols(k)] = high
            lift_one[x, size:, cols(k)] = low

    for i in range(clusters):
        for e in range(3):
            pos_ext[margin + i, e : e + 1] = pos_ref[e, i : i + 1]
        pos_ext[margin + i, 3:4] = species_ref[i : i + 1].astype(F32)
    pl.loop(margin, margin + clusters)(prepare)
    finish(pos_copies)
    for s in range(margin):
        pos_ext[s] = recv_pos[0, s]
        pos_ext[margin + clusters + s] = recv_pos[1, s]
    pl.loop(0, margin)(prepare)
    pl.loop(margin + clusters, ext)(prepare)

    eye = (
        lax.broadcasted_iota(jnp.int32, (size, size), 0)
        == lax.broadcasted_iota(jnp.int32, (size, size), 1)
    ).astype(F32)

    @pl.loop(0, cap)
    def _(t):
        center = tiles_ref[0, t]
        partner = tiles_ref[1, t]
        live = (t < count_ref[0]).astype(F32)
        same = live * (partner == center + margin).astype(F32)
        here = pos_ext[center + margin]
        u = [spread_pos[partner, e] - here[e : e + 1] for e in range(3)]
        square = u[0] * u[0] + u[1] * u[1] + u[2] * u[2] + soften
        inverse = lax.rsqrt(square)
        rho = square * inverse
        inside = jnp.maximum(1.0 - square * (1.0 / cutoff**2), 0.0)
        x = (rho - first_center) * (1.0 / spread)
        phi = jnp.exp(-x * x) * (inside * inside) * (live - same * eye)
        step = jnp.exp((2.0 * ratio) * x)
        y = [c * inverse for c in u]
        safe = jnp.where(inside > 0.0, inside, 1.0)
        slope = jnp.where(inside > 0.0, (-4.0 / cutoff**2) * rho / safe, 0.0)
        direction[t, 0] = y[0]
        direction[t, 1] = y[1]
        direction[t, 2] = y[2]
        direction[t, 3] = inverse
        direction[t, 4] = slope - (2.0 / spread) * x
        for k in range(bases):
            scaled = phi * math.exp(-((k * ratio) ** 2))
            radial[t, k] = scaled
            kern[t, 0, k] = scaled.astype(BF16)
            for m in range(3):
                kern[t, 1 + m, k] = (scaled * y[m]).astype(BF16)
            if k + 1 < bases:
                phi = phi * step

        before = links[0, t]
        for m in range(0, 4, 2):
            parts = None
            for k in range(0, bases, 2):
                block = jnp.concatenate(
                    [
                        jnp.concatenate([kern[t, m, k], kern[t, m + 1, k]], axis=1),
                        jnp.concatenate([kern[t, m, k + 1], kern[t, m + 1, k + 1]], axis=1),
                    ],
                    axis=0,
                )
                part = dot(lift_one[partner, :, cols(k, 2)], block)
                parts = part if parts is None else parts + part
            total[t, :, cols(m, 2)] = total[before, :, cols(m, 2)] + (parts[0:size] + parts[size:])

    mix_one_t = mix_one_ref[...].astype(F32).T.astype(BF16)
    mix_two_t = mix_two_ref[...].astype(F32).T.astype(BF16)

    @pl.loop(0, clusters)
    def _(g):
        last = links[2, g]
        mixed = dot(mix_one_t, total[last].astype(BF16))
        layer_t[margin + g, :, cols(0)] = (mixed[:, cols(0)] + feat_t[margin + g]).astype(BF16)
        layer_t[margin + g, :, cols(1, 3)] = mixed[:, cols(1, 3)].astype(BF16)

    for side in range(2):
        for s in range(margin):
            send_feat[side, s] = layer_t[margin + border_ref[side, s]]
    feat_dst = (recv_feat.at[0], recv_feat.at[1])
    feat_copies = exchange(1, send_feat.at[0], send_feat.at[1], feat_dst)

    def turn(x):
        for m in range(4):
            layer[x, m] = layer_t[x, :, cols(m)].astype(F32).T.astype(BF16)

    @pl.loop(0, clusters)
    def _(g):
        turn(margin + g)
        for m in range(4):
            desc_ref[g, m] = layer[margin + g, m]

    finish(feat_copies)
    for s in range(margin):
        layer_t[s] = recv_feat[0, s]
        layer_t[margin + clusters + s] = recv_feat[1, s]

    @pl.loop(0, cap)
    def _(t):
        partner = tiles_ref[1, t]
        message = second[links[0, t]]
        for k in range(0, bases, 2):
            parts = None
            for m in range(0, 4, 2):
                block = jnp.concatenate(
                    [
                        jnp.concatenate([kern[t, m, k], kern[t, m, k + 1]], axis=1),
                        jnp.concatenate([kern[t, m + 1, k], kern[t, m + 1, k + 1]], axis=1),
                    ],
                    axis=0,
                )
                part = dot(layer_t[partner, :, cols(m, 2)], block)
                parts = part if parts is None else parts + part
            message = message + scale_two[k] * parts[:, cols(0)] + scale_two[k + 1] * parts[:, cols(1)]
        second[t] = message

    readout_wide = spread_row(readout_ref[...].astype(F32))

    @pl.loop(0, clusters)
    def _(g):
        last = links[2, g]
        activation = dot(mix_two_t, second[last].astype(BF16))
        activation = activation + layer_t[margin + g, :, cols(0)].astype(F32)
        for m in range(1, 4):
            vector = layer_t[margin + g, :, cols(m)].astype(F32)
            activation = activation + vector * vector
        sigmoid = 1.0 / (1.0 + jnp.exp(-activation))
        energy_ref[pl.ds(g, 1)] = jnp.sum(
            activation * sigmoid * readout_wide, axis=0, keepdims=True
        )
        energy_t = readout_wide * sigmoid * (1.0 + activation * (1.0 - sigmoid))
        high, low = split(energy_t)
        adjoint_t = dot(mix_two_ref[...], high) + dot(mix_two_ref[...], low)
        adjoint = adjoint_t.T
        for k in range(bases):
            adj_two_t[g, :, cols(k)] = (scale_two[k] * adjoint_t).astype(BF16)
            adj_two[g, cols(k), :] = (
                (message_scale * radial_two_ref[k : k + 1]) * adjoint
            ).astype(BF16)
        energy_grad = energy_t.T
        direct[g, cols(0), :] = energy_grad
        for m in range(1, 4):
            direct[g, cols(m), :] = 2.0 * layer[margin + g, m].astype(F32) * energy_grad

    @pl.loop(0, cap)
    def _(t):
        center = tiles_ref[0, t]
        before = links[1, t]
        for m in range(4):
            parts = None
            for k in range(0, bases, 2):
                block = jnp.concatenate([kern[t, m, k], kern[t, m, k + 1]], axis=1)
                part = dot(block, adj_two[center, cols(k, 2), :])
                parts = part if parts is None else parts + part
            total[t, :, cols(m)] = total[before, :, cols(m)] + parts

    for side, start in enumerate((0, margin + clusters)):
        for s in range(margin):
            send_grad[side, s] = total[links[3, start + s]].astype(BF16)
    grad_dst = (recv_grad.at[0, pl.ds(0, margin)], recv_grad.at[1, pl.ds(0, margin)])
    grad_copies = exchange(2, send_grad.at[0], send_grad.at[1], grad_dst)
    pl.loop(0, margin)(turn)
    pl.loop(margin + clusters, ext)(turn)
    finish(grad_copies)

    @pl.loop(0, clusters)
    def _(g):
        last = links[3, margin + g]
        from_left = links[4, g]
        from_right = links[5, g]
        for m in range(4):
            grad = (
                direct[g, cols(m), :]
                + total[last, :, cols(m)]
                + recv_grad[0, from_left, :, cols(m)].astype(F32)
                + recv_grad[1, from_right, :, cols(m)].astype(F32)
            )
            high, low = split(grad)
            first_t = dot(mix_one_ref[...], high, NT) + dot(mix_one_ref[...], low, NT)
            for k in range(bases):
                adj_one_t[g, m, :, cols(k)] = (scale_one[k] * first_t).astype(BF16)

    rows8 = lax.broadcasted_iota(jnp.int32, moves.shape, 0)

    @pl.loop(0, cap)
    def _(t):
        center = tiles_ref[0, t]
        partner = tiles_ref[1, t]
        y = [direction[t, e] for e in range(3)]
        lhs = [jnp.concatenate([layer[partner, m], feat[partner]], axis=1) for m in range(4)]
        along = jnp.zeros((size, size), F32)
        ramp = jnp.zeros((size, size), F32)
        across = [jnp.zeros((size, size), F32) for _ in range(3)]
        for k in reversed(range(0, bases, 2)):
            grads = []
            for m in range(4):
                rhs = jnp.concatenate(
                    [adj_two_t[center, :, cols(k, 2)], adj_one_t[center, m, :, cols(k, 2)]], axis=0
                )
                grads.append(dot(lhs[m], rhs))
            for j in (1, 0):
                phi = radial[t, k + j]
                part = [grad[:, cols(j)] for grad in grads]
                mixed = part[0] + y[0] * part[1] + y[1] * part[2] + y[2] * part[3]
                along = along + phi * mixed
                if k + j:
                    ramp = ramp + along
                for e in range(3):
                    across[e] = across[e] + phi * part[1 + e]
        inverse = direction[t, 3]
        stretch = along * direction[t, 4] + (2.0 * ratio / spread) * ramp
        stretch = stretch - inverse * (y[0] * across[0] + y[1] * across[1] + y[2] * across[2])
        at_center = []
        at_partner = []
        for e in range(3):
            pull = stretch * y[e] + inverse * across[e]
            at_center.append(jnp.sum(pull, axis=0, keepdims=True))
            at_partner.append(jnp.sum(pull.T, axis=0, keepdims=True))
        pad = jnp.zeros((5, size), F32)
        gone = jnp.concatenate(at_center + [pad], axis=0)
        came = jnp.concatenate(at_partner + [pad], axis=0)
        moves[...] = (
            moves[...]
            - jnp.where(rows8 == center + margin, gone[None], 0.0)
            + jnp.where(rows8 == partner, came[None], 0.0)
        )

    move_dst = (recv_move.at[0, pl.ds(0, margin)], recv_move.at[1, pl.ds(0, margin)])
    move_copies = exchange(
        3, moves.at[pl.ds(0, margin)], moves.at[pl.ds(margin + clusters, margin)], move_dst
    )
    finish(move_copies)
    for g in range(clusters):
        moved = moves[margin + g] + recv_move[0, links[4, g]] + recv_move[1, links[5, g]]
        for e in range(3):
            forces_ref[e, g : g + 1] = -moved[e : e + 1]


def shards(
    n,
    positions,
    species,
    element_embed,
    radial_one,
    mix_one,
    radial_two,
    mix_two,
    readout,
    tile_list,
    tile_count,
    border,
):
    clusters, _, size = positions.shape
    channels = element_embed.shape[1]
    bases = radial_one.shape[0]
    margin = border.shape[1]
    cap = tile_list.shape[0]
    ext = clusters + 2 * margin
    smem = pl.BlockSpec(memory_space=pltpu.SMEM)
    vmem = pl.BlockSpec(memory_space=pltpu.VMEM)
    hbm = pl.BlockSpec(memory_space=pltpu.HBM)
    arrays = (
        jnp.transpose(positions, (1, 0, 2)),
        species,
        element_embed,
        radial_one,
        mix_one,
        radial_two,
        mix_two,
        readout.reshape(1, channels),
    )
    square = (size, size)
    wide = 4 * size
    energy, forces, descriptors = pl.pallas_call(
        functools.partial(body, (n, clusters, margin, cap, bases, size)),
        out_shape=(
            jax.ShapeDtypeStruct((clusters, size), F32),
            jax.ShapeDtypeStruct((3, clusters, size), F32),
            jax.ShapeDtypeStruct((clusters, 4, size, channels), BF16),
        ),
        in_specs=[smem] * 3 + [hbm] * len(arrays),
        out_specs=(vmem, vmem, vmem),
        scratch_shapes=[
            pltpu.SMEM((6, 16), jnp.int32),
            *[pltpu.VMEM(array.shape, array.dtype) for array in arrays],
            pltpu.SemaphoreType.DMA((len(arrays),)),
            pltpu.VMEM((2, margin, 4, size), F32),
            pltpu.VMEM((2, margin, 4, size), F32),
            pltpu.VMEM((2, margin, channels, wide), BF16),
            pltpu.VMEM((2, margin, channels, wide), BF16),
            pltpu.VMEM((2, margin, size, wide), BF16),
            pltpu.VMEM((2, margin + 1, size, wide), BF16),
            pltpu.VMEM((2, margin + 1, 8, size), F32),
            pltpu.VMEM((ext, 4, size), F32),
            pltpu.VMEM((ext, 3) + square, F32),
            pltpu.VMEM((bases,) + square, F32),
            pltpu.VMEM((bases,) + square, F32),
            pltpu.VMEM((ext,) + square, F32),
            pltpu.VMEM((ext,) + square, BF16),
            pltpu.VMEM((ext, 2 * channels, bases * size), BF16),
            pltpu.VMEM((ext, channels, wide), BF16),
            pltpu.VMEM((ext, 4) + square, BF16),
            pltpu.VMEM((cap, 4, bases) + square, BF16),
            pltpu.VMEM((cap, bases) + square, F32),
            pltpu.VMEM((cap, 5) + square, F32),
            pltpu.VMEM((cap + 1, channels, wide), F32),
            pltpu.VMEM((cap + 1,) + square, F32),
            pltpu.VMEM((clusters, bases * size, channels), BF16),
            pltpu.VMEM((clusters, channels, bases * size), BF16),
            pltpu.VMEM((clusters, 4, channels, bases * size), BF16),
            pltpu.VMEM((clusters, wide, channels), F32),
            pltpu.VMEM((ext, 8, size), F32),
            pltpu.SemaphoreType.DMA((4, 2)),
            pltpu.SemaphoreType.DMA((4, 2)),
        ],
        compiler_params=pltpu.CompilerParams(
            collective_id=0, has_side_effects=True, vmem_limit_bytes=61 * 1024 * 1024
        ),
    )(
        tile_list.T,
        tile_count,
        border,
        *arrays,
    )
    return energy, jnp.transpose(forces, (1, 0, 2)), descriptors


def solution(mesh):
    placed = (
        P(("rep", "bx"), None, None),
        P(("rep", "bx"), None),
        P(),
        P(),
        P(),
        P(),
        P(),
        P(),
        P(("rep", "bx"), None),
        P(("rep", "bx")),
        P(("rep", "bx"), None),
    )
    return jax.shard_map(
        functools.partial(shards, mesh.shape["bx"]),
        mesh=mesh,
        in_specs=placed,
        out_specs=(
            P(("rep", "bx"), None),
            P(("rep", "bx"), None, None),
            P(("rep", "bx"), None, None, None),
        ),
        check_vma=False,
    )
```

```python
import functools
import math

import jax
import jax.numpy as jnp
from jax import lax
from jax.experimental import pallas as pl
from jax.experimental.pallas import tpu as pltpu
from jax.sharding import PartitionSpec as P

MESH = pl.DeviceIdType.MESH
F32 = jnp.float32
BF16 = jnp.bfloat16

soften = 0.25
cutoff = 3.6
spread = 0.9
first_center = 0.25
center_step = 0.45
message_scale = 0.125
ratio = center_step / spread

GROUP = 4
ROWS = 16

NN = (((1,), (0,)), ((), ()))
NT = (((1,), (1,)), ((), ()))
TN = (((0,), (0,)), ((), ()))


def dot(a, b, dims=NN):
    return lax.dot_general(a, b, dims, preferred_element_type=F32)


def split(value):
    high = value.astype(BF16)
    return high, (value - high.astype(F32)).astype(BF16)


def body(
    sizes,
    tiles_ref,
    count_ref,
    border_ref,
    pos_far,
    species_far,
    embed_far,
    radial_one_far,
    mix_one_far,
    radial_two_far,
    mix_two_far,
    readout_far,
    energy_ref,
    forces_ref,
    desc_ref,
    links,
    pos_ref,
    species_ref,
    embed_ref,
    radial_one_ref,
    mix_one_ref,
    radial_two_ref,
    mix_two_ref,
    readout_ref,
    load_sem,
    store_sem,
    send_pos,
    recv_pos,
    send_feat,
    recv_feat,
    send_grad,
    recv_grad,
    recv_move,
    pos_ext,
    spread_pos,
    scale_one,
    scale_two,
    feat_t,
    feat,
    lift_one,
    layer_t,
    layer,
    diagonal,
    grads_even,
    grads_odd,
    radial,
    direction,
    total,
    second,
    adj_two,
    adj_two_t,
    adj_one_t,
    direct,
    moves,
    send_sem,
    recv_sem,
    *kerns,
):
    n, clusters, margin, cap, bases, size = sizes
    group = len(kerns)
    rounds = cap // group
    ext = clusters + 2 * margin
    me = lax.axis_index("bx")
    rep = lax.axis_index("rep")
    right = lax.rem(me + 1, n)
    left = lax.rem(me + n - 1, n)

    def cols(i, width=1):
        return slice(i * size, (i + width) * size)

    def push(step, side, src, dst, piece=0):
        copy = pltpu.make_async_remote_copy(
            src_ref=src,
            dst_ref=dst,
            send_sem=send_sem.at[step, side, piece],
            recv_sem=recv_sem.at[step, 1 - side, piece],
            device_id=(rep, (left, right)[side]),
            device_id_type=MESH,
        )
        copy.start()
        return copy

    def finish(copies):
        for copy in copies:
            copy.wait()

    far = (
        pos_far, species_far, embed_far, radial_one_far, mix_one_far, radial_two_far, mix_two_far, readout_far
    )
    near = (
        pos_ref, species_ref, embed_ref, radial_one_ref, mix_one_ref, radial_two_ref, mix_two_ref, readout_ref
    )
    loads = [
        pltpu.make_async_copy(src, dst, load_sem.at[i])
        for i, (src, dst) in enumerate(zip(far, near, strict=True))
    ]
    for load in loads:
        load.start()
    barrier = pltpu.get_barrier_semaphore()
    for neighbour in (left, right):
        pl.semaphore_signal(barrier, inc=1, device_id=(rep, neighbour), device_id_type=MESH)

    for load in loads:
        load.wait()
    for side in range(2):
        for s in range(margin):
            which = border_ref[side, s]
            for e in range(3):
                send_pos[side, s, e : e + 1] = pos_ref[e, pl.ds(which, 1)]
            send_pos[side, s, 3:4] = species_ref[pl.ds(which, 1)].astype(F32)
    pl.semaphore_wait(barrier, 2)
    pos_copies = [push(0, side, send_pos.at[side], recv_pos.at[1 - side]) for side in range(2)]

    centers = [tiles_ref[0, t] for t in range(cap)]
    partners = [tiles_ref[1, t] for t in range(cap)]
    none = jnp.int32(cap)
    for row, ids, how_many in ((0, centers, clusters), (1, partners, ext)):
        for t in range(cap):
            found = none
            for s in range(t):
                found = jnp.where(ids[s] == ids[t], jnp.int32(s), found)
            links[row, t] = found
        for g in range(how_many):
            found = none
            for s in range(cap):
                found = jnp.where(ids[s] == g, jnp.int32(s), found)
            links[2 + row, g] = found
    for side in range(2):
        for g in range(clusters):
            found = jnp.int32(margin)
            for s in range(margin):
                found = jnp.where(border_ref[side, s] == g, jnp.int32(s), found)
            links[4 + side, g] = found

    def spread_row(row):
        return jnp.broadcast_to(row, (size, size)).T

    for k in range(bases):
        scale_one[k] = message_scale * spread_row(radial_one_ref[k : k + 1])
        scale_two[k] = message_scale * spread_row(radial_two_ref[k : k + 1])
    total[cap] = jnp.zeros(total.shape[1:], F32)
    second[cap] = jnp.zeros(second.shape[1:], F32)
    for side in range(2):
        recv_grad[side, margin] = jnp.zeros(recv_grad.shape[2:], BF16)
        recv_move[side, margin] = jnp.zeros(recv_move.shape[2:], F32)
    moves[...] = jnp.zeros(moves.shape, F32)
    kinds = embed_ref.shape[0]
    kind_row = lax.broadcasted_iota(jnp.int32, (kinds, size), 0)

    def prepare(x):
        here = pos_ext[x]
        for e in range(3):
            spread_pos[x, e] = spread_row(here[e : e + 1])
        onehot = (kind_row == here[3:4].astype(jnp.int32)).astype(F32).astype(BF16)
        first = dot(embed_ref[...], onehot, TN)
        feat_t[x] = first
        feat[x] = first.T.astype(BF16)
        for k in range(bases):
            high, low = split(scale_one[k] * first)
            lift_one[x, 0:size, cols(k)] = high
            lift_one[x, size:, cols(k)] = low

    for i in range(clusters):
        for e in range(3):
            pos_ext[margin + i, e : e + 1] = pos_ref[e, i : i + 1]
        pos_ext[margin + i, 3:4] = species_ref[i : i + 1].astype(F32)
    pl.loop(margin, margin + clusters)(prepare)
    finish(pos_copies)
    for s in range(margin):
        pos_ext[s] = recv_pos[0, s]
        pos_ext[margin + clusters + s] = recv_pos[1, s]
    pl.loop(0, margin)(prepare)
    pl.loop(margin + clusters, ext)(prepare)

    diagonal[...] = (
        lax.broadcasted_iota(jnp.int32, (size, size), 0)
        == lax.broadcasted_iota(jnp.int32, (size, size), 1)
    ).astype(F32)

    def pair(t):
        center = tiles_ref[0, t]
        partner = tiles_ref[1, t]
        live = (t < count_ref[0, 0]).astype(F32)
        same = live * (partner == center + margin).astype(F32)
        return center, partner, live, same

    def geometry(center, partner, live, same, rows):
        here = pos_ext[center + margin]
        u = [spread_pos[partner, e, rows] - here[e : e + 1] for e in range(3)]
        square = u[0] * u[0] + u[1] * u[1] + u[2] * u[2] + soften
        inverse = lax.rsqrt(square)
        rho = square * inverse
        inside = jnp.maximum(1.0 - square * (1.0 / cutoff**2), 0.0)
        x = (rho - first_center) * (1.0 / spread)
        phi = jnp.exp(-x * x) * (inside * inside) * (live - same * diagonal[rows])
        step = jnp.exp((2.0 * ratio) * x)
        scaled = []
        for k in range(bases):
            scaled.append(phi * math.exp(-((k * ratio) ** 2)))
            phi = phi * step
        return scaled, [c * inverse for c in u], inverse, rho, inside, x

    blocks = [slice(r, r + ROWS) for r in range(0, size, ROWS)]

    @pl.loop(0, rounds)
    def _(i):
        def form(j):
            what = pair(i * group + j)
            for rows in blocks:
                scaled, y = geometry(*what, rows)[:2]
                for k in range(bases):
                    kerns[j][i, 0, k, rows] = scaled[k].astype(BF16)
                    for m in range(3):
                        kerns[j][i, 1 + m, k, rows] = (scaled[k] * y[m]).astype(BF16)

        def gather(j):
            t = i * group + j
            kern = kerns[j]
            partner = tiles_ref[1, t]
            before = links[0, t]
            for m in range(0, 4, 2):
                parts = None
                for k in range(0, bases, 2):
                    block = jnp.concatenate(
                        [
                            jnp.concatenate([kern[i, m, k], kern[i, m + 1, k]], axis=1),
                            jnp.concatenate([kern[i, m, k + 1], kern[i, m + 1, k + 1]], axis=1),
                        ],
                        axis=0,
                    )
                    part = dot(lift_one[partner, :, cols(k, 2)], block)
                    parts = part if parts is None else parts + part
                total[t, :, cols(m, 2)] = total[before, :, cols(m, 2)] + (parts[0:size] + parts[size:])

        form(0)
        for j in range(group):
            if j + 1 < group:
                form(j + 1)
            gather(j)

    mix_one_t = mix_one_ref[...].astype(F32).T.astype(BF16)
    mix_two_t = mix_two_ref[...].astype(F32).T.astype(BF16)

    def layer_of(g, out):
        mixed = dot(mix_one_t, total[links[2, g]].astype(BF16))
        out[:, cols(0)] = (mixed[:, cols(0)] + feat_t[margin + g]).astype(BF16)
        out[:, cols(1, 3)] = mixed[:, cols(1, 3)].astype(BF16)

    feat_copies = []
    for s in range(margin):
        for side in range(2):
            layer_of(border_ref[side, s], send_feat.at[side, s])
        for side in range(2):
            feat_copies.append(push(1, side, send_feat.at[side, s], recv_feat.at[1 - side, s], s))

    @pl.loop(0, clusters)
    def _(g):
        layer_of(g, layer_t.at[margin + g])

    def turn(x):
        for m in range(4):
            layer[x, m] = layer_t[x, :, cols(m)].astype(F32).T.astype(BF16)

    @pl.loop(0, clusters)
    def _(g):
        turn(margin + g)

    store = pltpu.make_async_copy(layer.at[pl.ds(margin, clusters)], desc_ref, store_sem)
    store.start()

    @pl.loop(0, cap)
    def _(t):
        what = pair(t)
        for rows in blocks:
            scaled, y, inverse, rho, inside, x = geometry(*what, rows)
            safe = jnp.where(inside > 0.0, inside, 1.0)
            slope = jnp.where(inside > 0.0, (-4.0 / cutoff**2) * rho / safe, 0.0)
            for k in range(bases):
                radial[t, k, rows] = scaled[k]
            for e in range(3):
                direction[t, e, rows] = y[e]
            direction[t, 3, rows] = inverse
            direction[t, 4, rows] = slope - (2.0 / spread) * x

    finish(feat_copies)
    for s in range(margin):
        layer_t[s] = recv_feat[0, s]
        layer_t[margin + clusters + s] = recv_feat[1, s]

    @pl.loop(0, rounds)
    def _(i):
        for j in range(group):
            t = i * group + j
            kern = kerns[j]
            partner = tiles_ref[1, t]
            message = None
            for k in range(0, bases, 2):
                parts = None
                for m in range(0, 4, 2):
                    block = jnp.concatenate(
                        [
                            jnp.concatenate([kern[i, m, k], kern[i, m, k + 1]], axis=1),
                            jnp.concatenate([kern[i, m + 1, k], kern[i, m + 1, k + 1]], axis=1),
                        ],
                        axis=0,
                    )
                    part = dot(layer_t[partner, :, cols(m, 2)], block)
                    parts = part if parts is None else parts + part
                more = scale_two[k] * parts[:, cols(0)] + scale_two[k + 1] * parts[:, cols(1)]
                message = more if message is None else message + more
            second[t] = second[links[0, t]] + message

    readout_wide = spread_row(readout_ref[...].astype(F32))

    @pl.loop(0, clusters)
    def _(g):
        last = links[2, g]
        activation = dot(mix_two_t, second[last].astype(BF16))
        activation = activation + layer_t[margin + g, :, cols(0)].astype(F32)
        for m in range(1, 4):
            vector = layer_t[margin + g, :, cols(m)].astype(F32)
            activation = activation + vector * vector
        sigmoid = 1.0 / (1.0 + jnp.exp(-activation))
        energy_ref[pl.ds(g, 1)] = jnp.sum(
            activation * sigmoid * readout_wide, axis=0, keepdims=True
        )
        energy_t = readout_wide * sigmoid * (1.0 + activation * (1.0 - sigmoid))
        high, low = split(energy_t)
        adjoint_t = dot(mix_two_ref[...], high) + dot(mix_two_ref[...], low)
        adjoint = adjoint_t.T
        for k in range(bases):
            adj_two_t[g, :, cols(k)] = (scale_two[k] * adjoint_t).astype(BF16)
            adj_two[g, cols(k), :] = (
                (message_scale * radial_two_ref[k : k + 1]) * adjoint
            ).astype(BF16)
        energy_grad = energy_t.T
        direct[g, cols(0), :] = energy_grad
        for m in range(1, 4):
            direct[g, cols(m), :] = 2.0 * layer[margin + g, m].astype(F32) * energy_grad

    @pl.loop(0, rounds)
    def _(i):
        for j in range(group):
            t = i * group + j
            kern = kerns[j]
            center = tiles_ref[0, t]
            before = links[1, t]
            for m in range(4):
                parts = None
                for k in range(0, bases, 2):
                    block = jnp.concatenate([kern[i, m, k], kern[i, m, k + 1]], axis=1)
                    part = dot(block, adj_two[center, cols(k, 2), :])
                    parts = part if parts is None else parts + part
                total[t, :, cols(m)] = total[before, :, cols(m)] + parts

    for side, start in enumerate((0, margin + clusters)):
        for s in range(margin):
            send_grad[side, s] = total[links[3, start + s]].astype(BF16)
    grad_copies = [
        push(2, side, send_grad.at[side], recv_grad.at[1 - side, pl.ds(0, margin)]) for side in range(2)
    ]
    pl.loop(0, margin)(turn)
    pl.loop(margin + clusters, ext)(turn)
    finish(grad_copies)

    @pl.loop(0, clusters)
    def _(g):
        last = links[3, margin + g]
        from_left = links[4, g]
        from_right = links[5, g]
        for m in range(4):
            grad = (
                direct[g, cols(m), :]
                + total[last, :, cols(m)]
                + recv_grad[0, from_left, :, cols(m)].astype(F32)
                + recv_grad[1, from_right, :, cols(m)].astype(F32)
            )
            high, low = split(grad)
            first_t = dot(mix_one_ref[...], high, NT) + dot(mix_one_ref[...], low, NT)
            for k in range(bases):
                adj_one_t[g, m, :, cols(k)] = (scale_one[k] * first_t).astype(BF16)

    rows8 = lax.broadcasted_iota(jnp.int32, moves.shape, 0)

    def grads_of(t, out):
        center = tiles_ref[0, t]
        partner = tiles_ref[1, t]
        for m in range(4):
            lhs = jnp.concatenate([layer[partner, m], feat[partner]], axis=1)
            for k in range(0, bases, 2):
                rhs = jnp.concatenate(
                    [adj_two_t[center, :, cols(k, 2)], adj_one_t[center, m, :, cols(k, 2)]], axis=0
                )
                out[m, :, cols(k, 2)] = dot(lhs, rhs)

    def force(t, grads):
        center = tiles_ref[0, t]
        partner = tiles_ref[1, t]
        at_center = [None] * 3
        whole = [[], [], []]
        for rows in blocks:
            y = [direction[t, e, rows] for e in range(3)]
            along = ramp = None
            across = [None] * 3
            for k in reversed(range(bases)):
                phi = radial[t, k, rows]
                part = [grads[m, rows, cols(k)] for m in range(4)]
                mixed = phi * (part[0] + y[0] * part[1] + y[1] * part[2] + y[2] * part[3])
                along = mixed if along is None else along + mixed
                if k:
                    ramp = along if ramp is None else ramp + along
                for e in range(3):
                    pull = phi * part[1 + e]
                    across[e] = pull if across[e] is None else across[e] + pull
            inverse = direction[t, 3, rows]
            stretch = along * direction[t, 4, rows] + (2.0 * ratio / spread) * ramp
            stretch = stretch - inverse * (y[0] * across[0] + y[1] * across[1] + y[2] * across[2])
            for e in range(3):
                pull = stretch * y[e] + inverse * across[e]
                whole[e].append(pull)
                at_center[e] = pull if at_center[e] is None else at_center[e] + pull
        at_center = [jnp.sum(pull, axis=0, keepdims=True) for pull in at_center]
        at_partner = [
            jnp.sum(jnp.concatenate(pulls, axis=0).T, axis=0, keepdims=True) for pulls in whole
        ]
        pad = jnp.zeros((5, size), F32)
        gone = jnp.concatenate(at_center + [pad], axis=0)
        came = jnp.concatenate(at_partner + [pad], axis=0)
        moves[...] = (
            moves[...]
            + jnp.where(rows8 == partner, came[None], 0.0)
            - jnp.where(rows8 == center + margin, gone[None], 0.0)
        )

    grads_of(0, grads_even)

    @pl.loop(0, cap // 2)
    def _(i):
        t = 2 * i
        grads_of(t + 1, grads_odd)
        force(t, grads_even)
        grads_of(jnp.minimum(t + 2, cap - 1), grads_even)
        force(t + 1, grads_odd)

    starts = (0, margin + clusters)
    move_copies = [
        push(3, side, moves.at[pl.ds(starts[side], margin)], recv_move.at[1 - side, pl.ds(0, margin)])
        for side in range(2)
    ]
    store.wait()
    finish(move_copies)
    for g in range(clusters):
        moved = moves[margin + g] + recv_move[0, links[4, g]] + recv_move[1, links[5, g]]
        for e in range(3):
            forces_ref[e, g : g + 1] = -moved[e : e + 1]


def hand_over(*refs):
    for src, dst in zip(refs[:3], refs[3:], strict=True):
        dst[...] = src[...]


def shards(
    n,
    positions,
    species,
    element_embed,
    radial_one,
    mix_one,
    radial_two,
    mix_two,
    readout,
    tile_list,
    tile_count,
    border,
):
    clusters, _, size = positions.shape
    channels = element_embed.shape[1]
    bases = radial_one.shape[0]
    margin = border.shape[1]
    cap = tile_list.shape[0]
    ext = clusters + 2 * margin
    smem = pl.BlockSpec(memory_space=pltpu.SMEM)
    vmem = pl.BlockSpec(memory_space=pltpu.VMEM)
    hbm = pl.BlockSpec(memory_space=pltpu.HBM)
    arrays = (
        jnp.transpose(positions, (1, 0, 2)),
        species,
        element_embed,
        radial_one,
        mix_one,
        radial_two,
        mix_two,
        readout.reshape(1, channels),
    )
    square = (size, size)
    wide = 4 * size
    group = math.gcd(cap, GROUP)
    energy, forces, descriptors = pl.pallas_call(
        functools.partial(body, (n, clusters, margin, cap, bases, size)),
        out_shape=(
            jax.ShapeDtypeStruct((clusters, size), F32),
            jax.ShapeDtypeStruct((3, clusters, size), F32),
            jax.ShapeDtypeStruct((clusters, 4, size, channels), BF16),
        ),
        in_specs=[smem] * 3 + [hbm] * len(arrays),
        out_specs=(vmem, vmem, hbm),
        scratch_shapes=[
            pltpu.SMEM((6, 16), jnp.int32),
            *[pltpu.VMEM(array.shape, array.dtype) for array in arrays],
            pltpu.SemaphoreType.DMA((len(arrays),)),
            pltpu.SemaphoreType.DMA,
            pltpu.VMEM((2, margin, 4, size), F32),
            pltpu.VMEM((2, margin, 4, size), F32),
            pltpu.VMEM((2, margin, channels, wide), BF16),
            pltpu.VMEM((2, margin, channels, wide), BF16),
            pltpu.VMEM((2, margin, size, wide), BF16),
            pltpu.VMEM((2, margin + 1, size, wide), BF16),
            pltpu.VMEM((2, margin + 1, 8, size), F32),
            pltpu.VMEM((ext, 4, size), F32),
            pltpu.VMEM((ext, 3) + square, F32),
            pltpu.VMEM((bases,) + square, F32),
            pltpu.VMEM((bases,) + square, F32),
            pltpu.VMEM((ext,) + square, F32),
            pltpu.VMEM((ext,) + square, BF16),
            pltpu.VMEM((ext, 2 * channels, bases * size), BF16),
            pltpu.VMEM((ext, channels, wide), BF16),
            pltpu.VMEM((ext, 4) + square, BF16),
            pltpu.VMEM(square, F32),
            pltpu.VMEM((4, size, bases * size), F32),
            pltpu.VMEM((4, size, bases * size), F32),
            pltpu.VMEM((cap, bases) + square, F32),
            pltpu.VMEM((cap, 5) + square, F32),
            pltpu.VMEM((cap + 1, channels, wide), F32),
            pltpu.VMEM((cap + 1,) + square, F32),
            pltpu.VMEM((clusters, bases * size, channels), BF16),
            pltpu.VMEM((clusters, channels, bases * size), BF16),
            pltpu.VMEM((clusters, 4, channels, bases * size), BF16),
            pltpu.VMEM((clusters, wide, channels), F32),
            pltpu.VMEM((ext, 8, size), F32),
            pltpu.SemaphoreType.DMA((4, 2, margin)),
            pltpu.SemaphoreType.DMA((4, 2, margin)),
            *[pltpu.VMEM((cap // group, 4, bases) + square, BF16) for _ in range(group)],
        ],
        compiler_params=pltpu.CompilerParams(
            collective_id=0, has_side_effects=True, vmem_limit_bytes=61 * 1024 * 1024
        ),
    )(
        tile_list.T,
        tile_count.reshape(1, 1),
        border,
        *arrays,
    )
    results = (energy, forces, descriptors)
    energy, forces, descriptors = pl.pallas_call(
        hand_over,
        out_shape=tuple(jax.ShapeDtypeStruct(x.shape, x.dtype) for x in results),
        in_specs=[vmem] * 3,
        out_specs=(vmem, vmem, vmem),
    )(*results)
    return energy, jnp.transpose(forces, (1, 0, 2)), descriptors


def solution(mesh):
    placed = (
        P(("rep", "bx"), None, None),
        P(("rep", "bx"), None),
        P(),
        P(),
        P(),
        P(),
        P(),
        P(),
        P(("rep", "bx"), None),
        P(("rep", "bx")),
        P(("rep", "bx"), None),
    )
    return jax.shard_map(
        functools.partial(shards, mesh.shape["bx"]),
        mesh=mesh,
        in_specs=placed,
        out_specs=(
            P(("rep", "bx"), None),
            P(("rep", "bx"), None, None),
            P(("rep", "bx"), None, None, None),
        ),
        check_vma=False,
    )
```
